32 devices in a mesh: groups: 2 (over x), expert: 8 (over z, y), sub: 2 (over core).
Axes of the slice: x: 2, y: 2, z: 4, core: 2. Of those that a mesh axis runs over, the one named last changes fastest.
Arguments:
- hidden_state: bfloat16 [2048, 2048], P(('groups', 'expert', 'sub')), parts along dimension 0, may hold values from -6 to 6
- norm_gain: float32 [2048], replicated, may hold values from 0.5 to 1.5
- router_weight: bfloat16 [2048, 16], replicated, may hold values from -0.25 to 0.25
- expert_ids: int32 [2048, 6], P(('groups', 'expert', 'sub')), parts along dimension 0, may hold values from 0 to 15, all different within a row; in each aligned block of 64 rows (0 to 63, 64 to 127, ...) at most 32 rows name the same one
- live_counts: int32 [32], P(('groups', 'expert', 'sub')), parts along dimension 0, may hold values from 16 to 64
- routed_gate_up: bfloat16 [16, 2048, 2816], P(('expert', 'sub')), may hold values from -0.125 to 0.125
- routed_down: bfloat16 [16, 1408, 2048], P(('expert', 'sub')), may hold values from -0.15625 to 0.15625
- shared_weights: bfloat16 [3, 2048, 2816], P(None, None, 'expert'), may hold values from -0.125 to 0.125
Outputs:
- mixed: bfloat16 [2048, 2048], P(('groups', 'expert', 'sub')), parts along dimension 0
- penalty: float32 [2], P('groups'), parts along dimension 0
The draws below stay inside these ranges and needn't reach their ends.
There are 2 independent parts, one for each index of `groups`. The reference program is written for one: setup_inputs(seed, part) draws one part's arguments, and reference() takes and returns one part's arrays. A program takes and returns all parts, laid end to end along the dimension named above; an argument that names none is the same for every part. Nothing has to cross between parts.
Inputs may be any that keep to these rules, and one draw needn't show every extreme that they name: `expert_ids`: in each row the 6 experts differ; among the 64 rows of one device no expert is named more than 32 times.
All inputs are finite; a program needn't handle non-finite values.
Results may differ from the reference program's by a relative error of at most 0.0065.
Values may be sent and summed in bfloat16 or wider, within the bound.
A program may use at most 128 MiB of HBM per device.

```python
import math
import jax
import jax.numpy as jnp
import numpy as np
from jax import lax

D = 2048
FF = 1408
SHARED_FF = 2816
TOP = 6
TOK_DEV = 64
EXPERTS = 16
CAP = 32
TOKENS = 1024
N_EXPERT = 8
N_SUB = 2


def draw_live_counts(key, part):
    count = N_EXPERT * N_SUB
    lowest = max(TOK_DEV // 4, 1)
    spread = max(TOK_DEV // 8, 1)
    index = jnp.arange(count, dtype=jnp.int32)
    base = lowest + (TOK_DEV - lowest) * index // (count - 1)
    jitter = jax.random.randint(jax.random.fold_in(key, 17), (count,), -spread, spread + 1, dtype=jnp.int32)
    inner = ((index > 0) & (index < count - 1)).astype(jnp.int32)
    return jnp.clip(base + jitter * inner, lowest, TOK_DEV).astype(jnp.int32)


def level_of(rng, shape, cuts, low, largest):
    gain = 1.0
    for axis_at, blocks in cuts:
        heights = jax.random.uniform(jax.random.fold_in(jax.random.fold_in(rng, 6), axis_at), (blocks,), jnp.float32, low / len(cuts), largest / len(cuts))
        gain = gain * jnp.repeat(jnp.exp(heights), shape[axis_at] // blocks).reshape((-1,) + (1,) * (len(shape) - 1 - axis_at))
    return gain


def deal_out(key, own, number, rows, amount, top, limit, lean):
    order = jax.random.permutation(key, amount)
    crowded, ordinary = portions_of(amount, rows * top, limit, lean, True), portions_of(amount, rows * top, limit, lean, False)
    places = jnp.arange(amount)

    def named(sizes, rotation):
        used = int((sizes > 0).sum())
        fixed = max(1, used // 4)
        moved = fixed + (places - fixed + rotation * (used - fixed)) % max(1, amount - fixed)
        return jnp.zeros((amount,), jnp.int32).at[order[jnp.where(places < fixed, places, moved)]].set(jnp.asarray(sizes, jnp.int32))

    sizes = jnp.where(number % 4 == 0, named(crowded, number // 4), named(ordinary, number - number // 4 - 1))
    mixed = jax.random.permutation(jax.random.fold_in(own, 3), amount)
    donor, receiver = mixed[0:amount // 2 * 2:2], mixed[1:amount // 2 * 2:2]
    margin = jnp.minimum(sizes[donor] - 1, limit - sizes[receiver]) // 2
    margin = jnp.where((donor == order[0]) | (receiver == order[0]) | (sizes[receiver] == 0), 0, jnp.maximum(margin, 0))
    moved = jax.random.randint(jax.random.fold_in(own, 4), (amount // 2,), 0, 1 << 20) % (margin + 1)
    sizes = sizes.at[donor].add(-moved).at[receiver].add(moved)
    items = jnp.searchsorted(jnp.cumsum(sizes), jnp.arange(rows * top), side="right").astype(jnp.int32)
    listing = items.reshape(top, rows).T
    listing = listing[jax.random.permutation(jax.random.fold_in(own, 1), rows)]
    rotation = jax.random.randint(jax.random.fold_in(own, 2), (rows, 1), 0, top)
    return jnp.take_along_axis(listing, (jnp.arange(top)[None, :] + rotation) % top, axis=1)


def portions_of(count, total, bound, lean, full):
    loads = [(1 << 20) // math.isqrt(rank ** lean) + 1 for rank in range(1, count + 1)]
    largest = bound if full else min(bound, max(-(-total // count), total * loads[0] // sum(loads)))
    least = 1 if total - largest >= count - 1 else 0
    counts, rest = [largest] + [least] * (count - 1), total - largest - least * (count - 1)
    while rest > 0:
        candidates = [i for i in range(1, count) if counts[i] < largest] or [i for i in range(1, count) if counts[i] < bound]
        pool, left = sum([loads[i] for i in candidates]), rest
        for i in candidates:
            extra = min(bound - counts[i], max(1, left * loads[i] // pool), rest)
            counts[i] = counts[i] + extra
            rest = rest - extra
    return np.array(counts)


def scatter_about(stream_key, extent, scale, most, cuts=(), kind=jnp.bfloat16):
    level = level_of(stream_key, extent, cuts, -0.22, 0.18) if cuts else 1.0
    entries = jax.random.normal(stream_key, extent, jnp.float32) * scale * level
    return jnp.minimum(jnp.maximum(entries, -most), most).astype(kind)


def setup_inputs(seed: int = 0, part: int = 0) -> dict:
    keys = jax.random.split(jax.random.key(seed), 9)
    own_keys = jax.random.split(jax.random.fold_in(keys[8], part), 9)
    hidden_state = scatter_about(own_keys[0], (TOKENS, D), 1.0, 6.0, ((0, 16),))
    norm_gain = jnp.clip(1.0 + 0.1 * jax.random.normal(keys[1], (D,), jnp.float32), 0.5, 1.5)
    router_weight = scatter_about(keys[2], (D, EXPERTS), (D // 4) ** -0.5, 0.25)
    expert_ids_keys = jax.random.split(jax.random.fold_in(own_keys[3], 1), TOKENS // TOK_DEV)
    expert_ids_turns = jax.random.permutation(jax.random.fold_in(own_keys[3], 3), TOKENS // TOK_DEV)
    expert_ids = jax.vmap(lambda own, number: deal_out(jax.random.fold_in(own_keys[3], 2), own, number, TOK_DEV, EXPERTS, TOP, CAP, 1))(expert_ids_keys, expert_ids_turns).reshape((TOKENS, TOP))
    live_counts = draw_live_counts(jax.random.fold_in(jax.random.fold_in(keys[8], part), 71), part)
    routed_gate_up = scatter_about(keys[5], (EXPERTS, D, 2 * FF), D ** -0.5, 0.125, ((0, 16),))
    routed_down = scatter_about(keys[6], (EXPERTS, FF, D), FF ** -0.5, 0.15625, ((0, 16),))
    shared_weights = scatter_about(keys[7], (3, D, SHARED_FF), D ** -0.5, 0.125, ((2, 8),))
    return {"hidden_state": hidden_state, "norm_gain": norm_gain, "router_weight": router_weight, "expert_ids": expert_ids, "live_counts": live_counts, "routed_gate_up": routed_gate_up, "routed_down": routed_down, "shared_weights": shared_weights}


def normalize(states, norm_gain):
    values = states.astype(jnp.float32)
    spread = lax.optimization_barrier(jnp.mean(values * values, axis=-1, keepdims=True))
    return (values * lax.rsqrt(spread + 1e-06) * norm_gain).astype(jnp.bfloat16)

def expert_ffn(packed):
    inputs, gate_up, down_proj = packed
    inner = jnp.dot(inputs, gate_up, preferred_element_type=jnp.float32)
    active = (jax.nn.silu(inner[:, :FF]) * inner[:, FF:]).astype(jnp.bfloat16)
    return jnp.dot(active, down_proj, preferred_element_type=jnp.float32).astype(jnp.bfloat16)

def reference(hidden_state, norm_gain, router_weight, expert_ids, live_counts, routed_gate_up, routed_down, shared_weights):
    devices = N_EXPERT * N_SUB
    normed = normalize(hidden_state, norm_gain)
    probs = jax.nn.sigmoid(jnp.dot(normed, router_weight, preferred_element_type=jnp.float32))
    positions = jnp.arange(TOKENS, dtype=jnp.int32)
    owners = positions // TOK_DEV
    live = (positions % TOK_DEV < live_counts[owners]).astype(jnp.float32)
    columns = jnp.arange(EXPERTS, dtype=jnp.int32)
    onehot = (expert_ids[:, :, None] == columns[None, None, :]).astype(jnp.int32)
    picked = lax.optimization_barrier(jnp.sum(onehot.astype(jnp.float32) * probs[:, None, :], axis=-1))
    weights = (live[:, None] * picked / lax.optimization_barrier(jnp.sum(picked, axis=-1, keepdims=True))).astype(jnp.bfloat16)
    live_hot = onehot * live.astype(jnp.int32)[:, None, None]
    per_device = live_hot.reshape(devices, TOK_DEV * TOP, EXPERTS)
    ranks = jnp.cumsum(per_device, axis=1) - per_device
    slot = lax.optimization_barrier(jnp.sum(ranks * per_device, axis=-1)).reshape(devices, TOK_DEV, TOP)
    places = expert_ids.reshape(devices, TOK_DEV, TOP) * CAP + slot
    valid = live.reshape(devices, TOK_DEV, 1, 1)
    cells = jnp.arange(EXPERTS * CAP, dtype=jnp.int32)
    match = (places[..., None] == cells[None, None, None, :]).astype(jnp.float32)
    table = lax.optimization_barrier(jnp.sum(match, axis=2)) * valid[:, :, 0]
    buffer = jnp.einsum('dtc,dtf->dcf', table, normed.reshape(devices, TOK_DEV, D).astype(jnp.float32)).astype(jnp.bfloat16)
    buffer = buffer.reshape(devices, EXPERTS, CAP, D).transpose(1, 0, 2, 3).reshape(EXPERTS, devices * CAP, D)
    outputs = lax.map(expert_ffn, (buffer, routed_gate_up, routed_down))
    outputs = outputs.reshape(EXPERTS, devices, CAP, D).transpose(1, 0, 2, 3).reshape(devices, EXPERTS * CAP, D)
    mixing = lax.optimization_barrier(jnp.sum(match * weights.reshape(devices, TOK_DEV, TOP, 1).astype(jnp.float32), axis=2))
    routed = jnp.einsum('dtc,dcf->dtf', mixing, outputs.astype(jnp.float32)).reshape(TOKENS, D)
    gate_part = jnp.dot(normed, shared_weights[0], preferred_element_type=jnp.float32)
    up_part = jnp.dot(normed, shared_weights[1], preferred_element_type=jnp.float32)
    shared_active = (jax.nn.silu(gate_part) * up_part).astype(jnp.bfloat16)
    shared_out = lax.dot_general(shared_active, shared_weights[2], (((1,), (1,)), ((), ())), preferred_element_type=jnp.float32)
    mixed = (shared_out + routed).astype(jnp.bfloat16)
    load = lax.optimization_barrier(jnp.sum(live_hot.astype(jnp.float32), axis=(0, 1)))
    mass = lax.optimization_barrier(jnp.sum(probs * live[:, None], axis=0))
    penalty = EXPERTS * jnp.sum(load * mass) / (TOP * float(TOKENS) * float(TOKENS))
    return (mixed, penalty.reshape(1))
```

```python
import jax
import jax.numpy as jnp
from jax import lax
from jax.sharding import PartitionSpec as P

BOTH = ("expert", "sub")


def normalize(states, norm_gain):
    values = states.astype(jnp.float32)
    spread = jnp.mean(values * values, axis=-1, keepdims=True)
    return (values * lax.rsqrt(spread + 1e-06) * norm_gain).astype(jnp.bfloat16)


def on_device(
    hidden_state,
    norm_gain,
    router_weight,
    expert_ids,
    live_counts,
    routed_gate_up,
    routed_down,
    shared_weights,
):
    tok_rows, width = hidden_state.shape
    choose = expert_ids.shape[1]
    local_experts = routed_gate_up.shape[0]
    hidden_units = routed_down.shape[1]
    chips = lax.axis_size("expert")
    subs = lax.axis_size("sub")
    devices = chips * subs
    all_experts = local_experts * devices
    all_tokens = tok_rows * devices
    capacity = (tok_rows * choose * 4 + 3 * all_experts - 1) // (3 * all_experts)
    my_sub = lax.axis_index("sub")
    me = lax.axis_index("expert") * subs + my_sub

    normed = normalize(hidden_state, norm_gain)
    everyone = lax.all_gather(normed, BOTH, axis=0, tiled=True)
    probs = jax.nn.sigmoid(jnp.dot(normed, router_weight, preferred_element_type=jnp.float32))
    live = (jnp.arange(tok_rows, dtype=jnp.int32) < live_counts[0]).astype(jnp.float32)
    columns = jnp.arange(all_experts, dtype=jnp.int32)
    hot = jnp.sum((expert_ids[:, :, None] == columns[None, None, :]).astype(jnp.float32), axis=1)
    picked = hot * probs
    weights = live[:, None] * picked / jnp.sum(picked, axis=-1, keepdims=True)
    live_hot = hot * live[:, None]
    notes = jnp.concatenate([weights, live_hot, probs * live[:, None]], axis=-1)
    notes = lax.all_gather(notes, BOTH, axis=0, tiled=True)
    load = jnp.sum(notes[:, all_experts : 2 * all_experts], axis=0)
    mass = jnp.sum(notes[:, 2 * all_experts :], axis=0)
    penalty = all_experts * jnp.sum(load * mass) / (choose * float(all_tokens) * float(all_tokens))

    owner = jnp.arange(all_tokens, dtype=jnp.int32) // tok_rows
    cells = jnp.arange(devices * capacity, dtype=jnp.int32)
    mixed = None
    for item in range(local_experts):
        column = me * local_experts + item
        chosen = lax.dynamic_slice_in_dim(notes, all_experts + column, 1, axis=1)
        weight = lax.dynamic_slice_in_dim(notes, column, 1, axis=1).astype(jnp.bfloat16)
        by_owner = chosen.reshape(devices, tok_rows)
        before = jnp.arange(tok_rows)[:, None] < jnp.arange(tok_rows)[None, :]
        rank = jnp.dot(by_owner, before.astype(jnp.float32)).reshape(all_tokens)
        place = jnp.where(chosen[:, 0] > 0, rank.astype(jnp.int32) + owner * capacity, -1)
        match = place[:, None] == cells[None, :]
        table = match.astype(jnp.bfloat16)
        rows = lax.dot_general(
            table, everyone, (((0,), (0,)), ((), ())), preferred_element_type=jnp.float32
        ).astype(jnp.bfloat16)
        inner = jnp.dot(rows, routed_gate_up[item], preferred_element_type=jnp.float32)
        active = (jax.nn.silu(inner[:, :hidden_units]) * inner[:, hidden_units:]).astype(
            jnp.bfloat16
        )
        results = jnp.dot(active, routed_down[item], preferred_element_type=jnp.float32).astype(
            jnp.bfloat16
        )
        mixing = jnp.where(match, weight, jnp.zeros((), jnp.bfloat16))
        part = jnp.dot(mixing, results, preferred_element_type=jnp.float32)
        mixed = part if mixed is None else mixed + part

    piece = lax.dynamic_index_in_dim(
        everyone.reshape(chips, subs, tok_rows, width), my_sub, axis=1, keepdims=False
    ).reshape(chips * tok_rows, width)
    gate_part = jnp.dot(piece, shared_weights[0], preferred_element_type=jnp.float32)
    up_part = jnp.dot(piece, shared_weights[1], preferred_element_type=jnp.float32)
    shared_active = (jax.nn.silu(gate_part) * up_part).astype(jnp.bfloat16)
    partials = lax.dot_general(
        shared_active,
        shared_weights[2],
        (((1,), (1,)), ((), ())),
        preferred_element_type=jnp.float32,
    )
    mine = (jnp.arange(subs) == my_sub)[None, :, None, None]
    partials = jnp.where(mine, partials.reshape(chips, 1, tok_rows, width), 0.0)
    total = (mixed.reshape(chips, subs, tok_rows, width) + partials).astype(jnp.bfloat16)
    total = total.reshape(all_tokens, width)
    mixed = lax.psum_scatter(total, BOTH, scatter_dimension=0, tiled=True)
    return (mixed.astype(jnp.bfloat16), penalty.reshape(1))


def solution(mesh):
    placed = (
        P(("groups", "expert", "sub"), None),
        P(),
        P(),
        P(("groups", "expert", "sub"), None),
        P(("groups", "expert", "sub")),
        P(("expert", "sub"), None, None),
        P(("expert", "sub"), None, None),
        P(None, None, "expert"),
    )
    return jax.shard_map(
        on_device,
        mesh=mesh,
        in_specs=placed,
        out_specs=(P(("groups", "expert", "sub"), None), P("groups")),
        check_vma=False,
    )
```

```python
import functools

import jax
import jax.numpy as jnp
from jax import lax
from jax.experimental import pallas as pl
from jax.experimental.pallas import tpu as pltpu
from jax.sharding import PartitionSpec as P

MESH = pl.DeviceIdType.MESH


def ring_place(chip, chips, fold):
    if fold == 1:
        return chip
    row, step = chip % 2, chip // 2
    return (1 - row) * step + row * (chips - 1 - step)


def ring_chip(place, chips, fold):
    if fold == 1:
        return place
    back = place // (chips // 2)
    step = (1 - back) * place + back * (chips - 1 - place)
    return 2 * step + back


def neighbours(chips, subs, fold):
    sub = lax.axis_index("sub")
    chip = lax.axis_index("expert")
    place = ring_place(chip, chips, fold)
    right = ring_chip((place + 1) % chips, chips, fold)
    left = ring_chip((place + chips - 1) % chips, chips, fold)
    along = [{"expert": right, "sub": sub}, {"expert": left, "sub": sub}]
    peers = [{"expert": chip, "sub": (sub + i) % subs} for i in range(1, subs)]
    return along, peers


def greet(along, peers):
    barrier = pltpu.get_barrier_semaphore()
    for target in along + peers:
        pl.semaphore_signal(barrier, inc=1, device_id=target, device_id_type=MESH)
    pl.semaphore_wait(barrier, len(along) + len(peers))


def carried(chips, hop, way, pieces):
    if 2 * hop < chips:
        return range(pieces)
    if 2 * hop == chips:
        return [0, 2] if way == 0 else [1]
    return []


def gather_kernel(
    chips, subs, fold, block_ref, notes_ref, all_ref, all_notes_ref,
    ring_send, ring_recv, peer_send, peer_recv, own_sem,
):
    along, peers = neighbours(chips, subs, fold)
    rows = block_ref.shape[0]
    half = rows // 2
    hops = chips // 2

    def piece(r, k, j):
        if j == 2:
            return all_notes_ref.at[r, k % chips]
        return all_ref.at[r, k % chips, pl.ds(j * half, half)]

    def own_piece(j):
        if j == 2:
            return notes_ref
        return block_ref.at[pl.ds(j * half, half)]

    def ring_copy(way, hop, j):
        sign = -1 if way == 0 else 1
        source = own_piece(j) if hop == 1 else piece(0, sign * (hop - 1), j)
        return pltpu.make_async_remote_copy(
            src_ref=source,
            dst_ref=piece(0, sign * hop, j),
            send_sem=ring_send.at[way, hop - 1, j],
            recv_sem=ring_recv.at[way, hop - 1, j],
            device_id=along[way],
            device_id_type=MESH,
        )

    def peer_copy(i, k, j):
        source = own_piece(j) if k == 0 else piece(0, k, j)
        return pltpu.make_async_remote_copy(
            src_ref=source,
            dst_ref=piece(subs - i, k, j),
            send_sem=peer_send.at[i - 1, k % chips, j],
            recv_sem=peer_recv.at[i - 1, k % chips, j],
            device_id=peers[i - 1],
            device_id_type=MESH,
        )

    keep = [
        pltpu.make_async_copy(block_ref, all_ref.at[0, 0], own_sem.at[0]),
        pltpu.make_async_copy(notes_ref, all_notes_ref.at[0, 0], own_sem.at[1]),
    ]
    greet(along, peers)
    started, pending = [], []
    for j in (2, 0, 1):
        for way in range(2):
            if j in carried(chips, 1, way, 3):
                copy = ring_copy(way, 1, j)
                copy.start()
                started.append(copy)
    for j in range(3):
        for i in range(1, subs):
            copy = peer_copy(i, 0, j)
            copy.start()
            started.append(copy)
            pending.append(copy)
    for copy in keep:
        copy.start()
    for hop in range(1, hops + 1):
        for j in (2, 0, 1):
            for way in range(2):
                if j not in carried(chips, hop, way, 3):
                    continue
                ring_copy(way, hop, j).wait_recv()
                if j in carried(chips, hop + 1, way, 3):
                    copy = ring_copy(way, hop + 1, j)
                    copy.start()
                    started.append(copy)
                for i in range(1, subs):
                    copy = peer_copy(i, -hop if way == 0 else hop, j)
                    copy.start()
                    started.append(copy)
                    pending.append(copy)
    for copy in pending:
        copy.wait_recv()
    for copy in started:
        copy.wait_send()
    for copy in keep:
        copy.wait()


def scatter_kernel(
    chips, subs, fold, part_ref, out_ref, from_peer, going, coming,
    ring_send, ring_recv, peer_send, peer_recv,
):
    along, peers = neighbours(chips, subs, fold)
    rows = out_ref.shape[0]
    half = rows // 2
    hops = chips // 2

    def peer_copy(i, k):
        k = k % chips
        return pltpu.make_async_remote_copy(
            src_ref=part_ref.at[i, k],
            dst_ref=from_peer.at[i - 1, k],
            send_sem=peer_send.at[i - 1, k],
            recv_sem=peer_recv.at[i - 1, k],
            device_id=peers[i - 1],
            device_id_type=MESH,
        )

    def ring_copy(way, hop, j):
        spot = (way, hop - 1, pl.ds(j * half, half))
        return pltpu.make_async_remote_copy(
            src_ref=going.at[spot],
            dst_ref=coming.at[spot],
            send_sem=ring_send.at[way, hop - 1, j],
            recv_sem=ring_recv.at[way, hop - 1, j],
            device_id=along[way],
            device_id_type=MESH,
        )

    def local_sum(k, j):
        span = pl.ds(j * half, half)
        value = part_ref[0, k % chips, span, :].astype(jnp.float32)
        for i in range(1, subs):
            value = value + from_peer[i - 1, k % chips, span, :].astype(jnp.float32)
        return value

    greet(along, peers)
    order = []
    for hop in range(hops, 0, -1):
        for k in (hop, -hop):
            if k % chips not in order:
                order.append(k % chips)
    order.append(0)
    sent = []
    for k in order:
        for i in range(1, subs):
            copy = peer_copy(i, k)
            copy.start()
            sent.append(copy)
    here = set()

    def need(k):
        if k % chips not in here:
            here.add(k % chips)
            for i in range(1, subs):
                peer_copy(i, k).wait_recv()

    for hop in range(hops, 0, -1):
        for j in range(2):
            for way in range(2):
                if j not in carried(chips, hop, way, 2):
                    continue
                k = hop if way == 0 else -hop
                need(k)
                value = local_sum(k, j)
                if j in carried(chips, hop + 1, way, 2):
                    ring_copy(way, hop + 1, j).wait_recv()
                    value = value + coming[way, hop, pl.ds(j * half, half), :].astype(jnp.float32)
                going[way, hop - 1, pl.ds(j * half, half), :] = value.astype(going.dtype)
                copy = ring_copy(way, hop, j)
                copy.start()
                sent.append(copy)
    need(0)
    for j in range(2):
        value = local_sum(0, j)
        for way in range(2):
            if j in carried(chips, 1, way, 2):
                ring_copy(way, 1, j).wait_recv()
                value = value + coming[way, 0, pl.ds(j * half, half), :].astype(jnp.float32)
        out_ref[pl.ds(j * half, half), :] = value.astype(out_ref.dtype)
    for copy in sent:
        copy.wait_send()


def ring_gather(block, notes, chips, subs, fold):
    hops = max(chips // 2, 1)
    vmem = pl.BlockSpec(memory_space=pltpu.VMEM)
    return pl.pallas_call(
        functools.partial(gather_kernel, chips, subs, fold),
        out_shape=(
            jax.ShapeDtypeStruct((subs, chips) + block.shape, block.dtype),
            jax.ShapeDtypeStruct((subs, chips) + notes.shape, notes.dtype),
        ),
        in_specs=[vmem, vmem],
        out_specs=(vmem, vmem),
        scratch_shapes=[
            pltpu.SemaphoreType.DMA((2, hops, 3)),
            pltpu.SemaphoreType.DMA((2, hops, 3)),
            pltpu.SemaphoreType.DMA((max(subs - 1, 1), chips, 3)),
            pltpu.SemaphoreType.DMA((max(subs - 1, 1), chips, 3)),
            pltpu.SemaphoreType.DMA((2,)),
        ],
        compiler_params=pltpu.CompilerParams(collective_id=0, has_side_effects=True),
        name="ring_gather",
    )(block, notes)


def ring_scatter(part, chips, subs, fold):
    hops = max(chips // 2, 1)
    rows, width = part.shape[2:]
    vmem = pl.BlockSpec(memory_space=pltpu.VMEM)
    return pl.pallas_call(
        functools.partial(scatter_kernel, chips, subs, fold),
        out_shape=jax.ShapeDtypeStruct((rows, width), part.dtype),
        in_specs=[vmem],
        out_specs=vmem,
        scratch_shapes=[
            pltpu.VMEM((max(subs - 1, 1), chips, rows, width), part.dtype),
            pltpu.VMEM((2, hops, rows, width), part.dtype),
            pltpu.VMEM((2, hops, rows, width), part.dtype),
            pltpu.SemaphoreType.DMA((2, hops, 2)),
            pltpu.SemaphoreType.DMA((2, hops, 2)),
            pltpu.SemaphoreType.DMA((max(subs - 1, 1), chips)),
            pltpu.SemaphoreType.DMA((max(subs - 1, 1), chips)),
        ],
        compiler_params=pltpu.CompilerParams(collective_id=1, has_side_effects=True),
        name="ring_scatter",
    )(part)


def normalize(states, norm_gain):
    values = states.astype(jnp.float32)
    spread = jnp.mean(values * values, axis=-1, keepdims=True)
    return (values * lax.rsqrt(spread + 1e-06) * norm_gain).astype(jnp.bfloat16)


def on_device(
    fold,
    hidden_state,
    norm_gain,
    router_weight,
    expert_ids,
    live_counts,
    routed_gate_up,
    routed_down,
    shared_weights,
):
    tok_rows, width = hidden_state.shape
    choose = expert_ids.shape[1]
    local_experts = routed_gate_up.shape[0]
    hidden_units = routed_down.shape[1]
    chips = lax.axis_size("expert")
    subs = lax.axis_size("sub")
    devices = chips * subs
    all_experts = local_experts * devices
    all_tokens = tok_rows * devices
    capacity = (tok_rows * choose * 4 + 3 * all_experts - 1) // (3 * all_experts)
    sub = lax.axis_index("sub")
    chip = lax.axis_index("expert")
    me = chip * subs + sub

    normed = normalize(hidden_state, norm_gain)
    probs = jax.nn.sigmoid(jnp.dot(normed, router_weight, preferred_element_type=jnp.float32))
    live = (jnp.arange(tok_rows, dtype=jnp.int32) < live_counts[0]).astype(jnp.float32)
    columns = jnp.arange(all_experts, dtype=jnp.int32)
    hot = jnp.sum((expert_ids[:, :, None] == columns[None, None, :]).astype(jnp.float32), axis=1)
    picked = hot * probs
    weights = live[:, None] * picked / jnp.sum(picked, axis=-1, keepdims=True)
    gate = probs * live[:, None]
    high = gate.astype(jnp.bfloat16)
    low = (gate - high.astype(jnp.float32)).astype(jnp.bfloat16)
    notes = jnp.concatenate(
        [weights.astype(jnp.bfloat16), (hot * live[:, None]).astype(jnp.bfloat16), high, low], axis=-1
    )
    spare = -notes.shape[1] % 128
    notes = jnp.pad(notes, ((0, 0), (0, spare)))
    everyone, notes = ring_gather(normed, notes, chips, subs, fold)

    notes = notes.astype(jnp.float32)
    place = ring_place(chip, chips, fold)
    origin = (
        ring_chip((place + jnp.arange(chips)[None, :]) % chips, chips, fold) * subs
        + (sub + jnp.arange(subs)[:, None]) % subs
    ).reshape(devices)
    sums = jnp.sum(notes.reshape(devices, tok_rows, -1), axis=1)
    at = origin[None, :] == jnp.arange(devices)[:, None]
    sums = jnp.sum(jnp.where(at[:, :, None], sums[None], 0.0), axis=1)
    sums = jnp.sum(sums, axis=0)
    load = sums[all_experts : 2 * all_experts]
    mass = sums[2 * all_experts : 3 * all_experts] + sums[3 * all_experts : 4 * all_experts]
    penalty = all_experts * jnp.sum(load * mass) / (choose * float(all_tokens) * float(all_tokens))

    everyone = everyone.reshape(all_tokens, width)
    notes = notes.reshape(all_tokens, -1)
    lanes = jnp.arange(notes.shape[1])
    owner = jnp.arange(all_tokens, dtype=jnp.int32) // tok_rows
    cells = jnp.arange(devices * capacity, dtype=jnp.int32)
    before = (jnp.arange(tok_rows)[:, None] < jnp.arange(tok_rows)[None, :]).astype(jnp.float32)
    mixed = None
    for item in range(local_experts):
        column = me * local_experts + item
        weight = jnp.sum(jnp.where(lanes[None, :] == column, notes, 0.0), axis=1)
        chosen = jnp.sum(jnp.where(lanes[None, :] == all_experts + column, notes, 0.0), axis=1)
        rank = jnp.dot(chosen.reshape(devices, tok_rows), before).reshape(all_tokens)
        spot = jnp.where(chosen > 0, rank.astype(jnp.int32) + owner * capacity, -1)
        match = spot[:, None] == cells[None, :]
        table = match.astype(jnp.bfloat16)
        mixing = jnp.where(match, weight[:, None], 0.0).astype(jnp.bfloat16)
        table, mixing = lax.optimization_barrier((table, mixing))
        rows = lax.dot_general(
            table, everyone, (((0,), (0,)), ((), ())), preferred_element_type=jnp.float32
        ).astype(jnp.bfloat16)
        inner = jnp.dot(rows, routed_gate_up[item], preferred_element_type=jnp.float32)
        active = (jax.nn.silu(inner[:, :hidden_units]) * inner[:, hidden_units:]).astype(
            jnp.bfloat16
        )
        results = jnp.dot(active, routed_down[item], preferred_element_type=jnp.float32).astype(
            jnp.bfloat16
        )
        part = jnp.dot(mixing, results, preferred_element_type=jnp.float32)
        mixed = part if mixed is None else mixed + part

    piece = everyone[: chips * tok_rows]
    gate_part = jnp.dot(piece, shared_weights[0], preferred_element_type=jnp.float32)
    up_part = jnp.dot(piece, shared_weights[1], preferred_element_type=jnp.float32)
    shared_active = (jax.nn.silu(gate_part) * up_part).astype(jnp.bfloat16)
    partials = lax.dot_general(
        shared_active,
        shared_weights[2],
        (((1,), (1,)), ((), ())),
        preferred_element_type=jnp.float32,
    )
    near = (mixed[: chips * tok_rows] + partials).astype(jnp.bfloat16)
    far = mixed[chips * tok_rows :].astype(jnp.bfloat16)
    total = jnp.concatenate([near, far], axis=0).reshape(subs, chips, tok_rows, width)
    return (ring_scatter(total, chips, subs, fold), penalty.reshape(1))


def fold_of(mesh):
    chips = mesh.shape["expert"]
    try:
        spots = [tuple(d.coords) for d in mesh.devices[0, :, 0].flat]
    except (AttributeError, TypeError, ValueError):
        spots = []
    if chips % 2 or chips < 4:
        return 1
    if len(spots) == chips:
        apart = sum(abs(a - b) for a, b in zip(spots[0], spots[2]))
        return 2 if apart == 1 else 1
    return 1


def solution(mesh):
    placed = (
        P(("groups", "expert", "sub"), None),
        P(),
        P(),
        P(("groups", "expert", "sub"), None),
        P(("groups", "expert", "sub")),
        P(("expert", "sub"), None, None),
        P(("expert", "sub"), None, None),
        P(None, None, "expert"),
    )
    return jax.shard_map(
        functools.partial(on_device, fold_of(mesh)),
        mesh=mesh,
        in_specs=placed,
        out_specs=(P(("groups", "expert", "sub"), None), P("groups")),
        check_vma=False,
    )
```

```python
import functools

import jax
import jax.numpy as jnp
from jax import lax
from jax.experimental import pallas as pl
from jax.experimental.pallas import tpu as pltpu
from jax.sharding import PartitionSpec as P

MESH = pl.DeviceIdType.MESH


def ring_place(chip, chips, fold):
    if fold == 1:
        return chip
    row, step = chip % 2, chip // 2
    return (1 - row) * step + row * (chips - 1 - step)


def ring_chip(place, chips, fold):
    if fold == 1:
        return place
    back = place // (chips // 2)
    step = (1 - back) * place + back * (chips - 1 - place)
    return 2 * step + back


def neighbours(chips, subs, fold):
    sub = lax.axis_index("sub")
    chip = lax.axis_index("expert")
    place = ring_place(chip, chips, fold)
    right = ring_chip((place + 1) % chips, chips, fold)
    left = ring_chip((place + chips - 1) % chips, chips, fold)
    along = [{"expert": right, "sub": sub}, {"expert": left, "sub": sub}]
    peers = [{"expert": chip, "sub": (sub + i) % subs} for i in range(1, subs)]
    return along, peers


def greet(along, peers):
    barrier = pltpu.get_barrier_semaphore()
    for target in along + peers:
        pl.semaphore_signal(barrier, inc=1, device_id=target, device_id_type=MESH)
    pl.semaphore_wait(barrier, len(along) + len(peers))


def carried(chips, hop, way, pieces):
    if 2 * hop < chips:
        return range(pieces)
    if 2 * hop == chips:
        return [0, 2] if way == 0 else [1]
    return []


def gather_kernel(
    chips, subs, fold, block_ref, notes_ref, all_ref, all_notes_ref,
    ring_send, ring_recv, peer_send, peer_recv, own_sem,
):
    along, peers = neighbours(chips, subs, fold)
    rows = block_ref.shape[0]
    half = rows // 2
    hops = chips // 2

    def piece(r, k, j):
        if j == 2:
            return all_notes_ref.at[r, k % chips]
        return all_ref.at[r, k % chips, pl.ds(j * half, half)]

    def own_piece(j):
        if j == 2:
            return notes_ref
        return block_ref.at[pl.ds(j * half, half)]

    def ring_copy(way, hop, j):
        sign = -1 if way == 0 else 1
        source = own_piece(j) if hop == 1 else piece(0, sign * (hop - 1), j)
        return pltpu.make_async_remote_copy(
            src_ref=source,
            dst_ref=piece(0, sign * hop, j),
            send_sem=ring_send.at[way, hop - 1, j],
            recv_sem=ring_recv.at[way, hop - 1, j],
            device_id=along[way],
            device_id_type=MESH,
        )

    def peer_copy(i, k, j):
        source = own_piece(j) if k == 0 else piece(0, k, j)
        return pltpu.make_async_remote_copy(
            src_ref=source,
            dst_ref=piece(subs - i, k, j),
            send_sem=peer_send.at[i - 1, k % chips, j],
            recv_sem=peer_recv.at[i - 1, k % chips, j],
            device_id=peers[i - 1],
            device_id_type=MESH,
        )

    keep = [
        pltpu.make_async_copy(block_ref, all_ref.at[0, 0], own_sem.at[0]),
        pltpu.make_async_copy(notes_ref, all_notes_ref.at[0, 0], own_sem.at[1]),
    ]
    greet(along, peers)
    started, pending = [], []
    for j in (2, 0, 1):
        for way in range(2):
            if j in carried(chips, 1, way, 3):
                copy = ring_copy(way, 1, j)
                copy.start()
                started.append(copy)
    for j in range(3):
        for i in range(1, subs):
            copy = peer_copy(i, 0, j)
            copy.start()
            started.append(copy)
            pending.append(copy)
    for copy in keep:
        copy.start()
    for hop in range(1, hops + 1):
        for j in (2, 0, 1):
            for way in range(2):
                if j not in carried(chips, hop, way, 3):
                    continue
                ring_copy(way, hop, j).wait_recv()
                if j in carried(chips, hop + 1, way, 3):
                    copy = ring_copy(way, hop + 1, j)
                    copy.start()
                    started.append(copy)
                for i in range(1, subs):
                    copy = peer_copy(i, -hop if way == 0 else hop, j)
                    copy.start()
                    started.append(copy)
                    pending.append(copy)
    for copy in pending:
        copy.wait_recv()
    for copy in started:
        copy.wait_send()
    for copy in keep:
        copy.wait()


def scatter_kernel(
    chips, subs, fold, *refs,
):
    parts = refs[:subs]
    out_ref, from_peer, going, coming, ring_send, ring_recv, peer_send, peer_recv = refs[subs:]
    along, peers = neighbours(chips, subs, fold)
    rows = out_ref.shape[0]
    half = rows // 2
    hops = chips // 2

    def peer_copy(i, k):
        k = k % chips
        return pltpu.make_async_remote_copy(
            src_ref=parts[i].at[k],
            dst_ref=from_peer.at[i - 1, k],
            send_sem=peer_send.at[i - 1, k],
            recv_sem=peer_recv.at[i - 1, k],
            device_id=peers[i - 1],
            device_id_type=MESH,
        )

    def ring_copy(way, hop, j):
        spot = (way, hop - 1, pl.ds(j * half, half))
        return pltpu.make_async_remote_copy(
            src_ref=going.at[spot],
            dst_ref=coming.at[spot],
            send_sem=ring_send.at[way, hop - 1, j],
            recv_sem=ring_recv.at[way, hop - 1, j],
            device_id=along[way],
            device_id_type=MESH,
        )

    def local_sum(k, j):
        span = pl.ds(j * half, half)
        value = parts[0][k % chips, span, :].astype(jnp.float32)
        for i in range(1, subs):
            value = value + from_peer[i - 1, k % chips, span, :].astype(jnp.float32)
        return value

    greet(along, peers)
    order = []
    for hop in range(hops, 0, -1):
        for k in (hop, -hop):
            if k % chips not in order:
                order.append(k % chips)
    order.append(0)
    sent = []
    for k in order:
        for i in range(1, subs):
            copy = peer_copy(i, k)
            copy.start()
            sent.append(copy)
    here = set()

    def need(k):
        if k % chips not in here:
            here.add(k % chips)
            for i in range(1, subs):
                peer_copy(i, k).wait_recv()

    for hop in range(hops, 0, -1):
        for j in range(2):
            for way in range(2):
                if j not in carried(chips, hop, way, 2):
                    continue
                k = hop if way == 0 else -hop
                need(k)
                value = local_sum(k, j)
                if j in carried(chips, hop + 1, way, 2):
                    ring_copy(way, hop + 1, j).wait_recv()
                    value = value + coming[way, hop, pl.ds(j * half, half), :].astype(jnp.float32)
                going[way, hop - 1, pl.ds(j * half, half), :] = value.astype(going.dtype)
                copy = ring_copy(way, hop, j)
                copy.start()
                sent.append(copy)
    need(0)
    for j in range(2):
        value = local_sum(0, j)
        for way in range(2):
            if j in carried(chips, 1, way, 2):
                ring_copy(way, 1, j).wait_recv()
                value = value + coming[way, 0, pl.ds(j * half, half), :].astype(jnp.float32)
        out_ref[pl.ds(j * half, half), :] = value.astype(out_ref.dtype)
    for copy in sent:
        copy.wait_send()


def ring_gather(block, notes, chips, subs, fold):
    hops = max(chips // 2, 1)
    vmem = pl.BlockSpec(memory_space=pltpu.VMEM)
    return pl.pallas_call(
        functools.partial(gather_kernel, chips, subs, fold),
        out_shape=(
            jax.ShapeDtypeStruct((subs, chips) + block.shape, block.dtype),
            jax.ShapeDtypeStruct((subs, chips) + notes.shape, notes.dtype),
        ),
        in_specs=[vmem, vmem],
        out_specs=(vmem, vmem),
        scratch_shapes=[
            pltpu.SemaphoreType.DMA((2, hops, 3)),
            pltpu.SemaphoreType.DMA((2, hops, 3)),
            pltpu.SemaphoreType.DMA((max(subs - 1, 1), chips, 3)),
            pltpu.SemaphoreType.DMA((max(subs - 1, 1), chips, 3)),
            pltpu.SemaphoreType.DMA((2,)),
        ],
        compiler_params=pltpu.CompilerParams(collective_id=0, has_side_effects=True),
        name="ring_gather",
    )(block, notes)


def ring_scatter(parts, chips, subs, fold):
    hops = max(chips // 2, 1)
    rows, width = parts[0].shape[1:]
    vmem = pl.BlockSpec(memory_space=pltpu.VMEM)
    return pl.pallas_call(
        functools.partial(scatter_kernel, chips, subs, fold),
        out_shape=jax.ShapeDtypeStruct((rows, width), parts[0].dtype),
        in_specs=[vmem] * subs,
        out_specs=vmem,
        scratch_shapes=[
            pltpu.VMEM((max(subs - 1, 1), chips, rows, width), parts[0].dtype),
            pltpu.VMEM((2, hops, rows, width), parts[0].dtype),
            pltpu.VMEM((2, hops, rows, width), parts[0].dtype),
            pltpu.SemaphoreType.DMA((2, hops, 2)),
            pltpu.SemaphoreType.DMA((2, hops, 2)),
            pltpu.SemaphoreType.DMA((max(subs - 1, 1), chips)),
            pltpu.SemaphoreType.DMA((max(subs - 1, 1), chips)),
        ],
        compiler_params=pltpu.CompilerParams(collective_id=1, has_side_effects=True),
        name="ring_scatter",
    )(*parts)


def normalize(states, norm_gain):
    values = states.astype(jnp.float32)
    spread = jnp.mean(values * values, axis=-1, keepdims=True)
    return (values * lax.rsqrt(spread + 1e-06) * norm_gain).astype(jnp.bfloat16)


def on_device(
    fold,
    hidden_state,
    norm_gain,
    router_weight,
    expert_ids,
    live_counts,
    routed_gate_up,
    routed_down,
    shared_weights,
):
    tok_rows, width = hidden_state.shape
    choose = expert_ids.shape[1]
    local_experts = routed_gate_up.shape[0]
    hidden_units = routed_down.shape[1]
    chips = lax.axis_size("expert")
    subs = lax.axis_size("sub")
    devices = chips * subs
    all_experts = local_experts * devices
    all_tokens = tok_rows * devices
    capacity = (tok_rows * choose * 4 + 3 * all_experts - 1) // (3 * all_experts)
    sub = lax.axis_index("sub")
    chip = lax.axis_index("expert")
    me = chip * subs + sub

    normed = normalize(hidden_state, norm_gain)
    probs = jax.nn.sigmoid(jnp.dot(normed, router_weight, preferred_element_type=jnp.float32))
    live = (jnp.arange(tok_rows, dtype=jnp.int32) < live_counts[0]).astype(jnp.float32)
    columns = jnp.arange(all_experts, dtype=jnp.int32)
    hot = jnp.sum((expert_ids[:, :, None] == columns[None, None, :]).astype(jnp.float32), axis=1)
    picked = hot * probs
    weights = live[:, None] * picked / jnp.sum(picked, axis=-1, keepdims=True)
    gate = probs * live[:, None]
    high = gate.astype(jnp.bfloat16)
    low = (gate - high.astype(jnp.float32)).astype(jnp.bfloat16)
    notes = jnp.concatenate(
        [weights.astype(jnp.bfloat16), (hot * live[:, None]).astype(jnp.bfloat16), high, low], axis=-1
    )
    spare = -notes.shape[1] % 128
    notes = jnp.pad(notes, ((0, 0), (0, spare)))
    everyone, notes = ring_gather(normed, notes, chips, subs, fold)

    notes = notes.astype(jnp.float32)
    place = ring_place(chip, chips, fold)
    origin = (
        ring_chip((place + jnp.arange(chips)[None, :]) % chips, chips, fold) * subs
        + (sub + jnp.arange(subs)[:, None]) % subs
    ).reshape(devices)
    sums = jnp.sum(notes.reshape(devices, tok_rows, -1), axis=1)
    at = origin[None, :] == jnp.arange(devices)[:, None]
    sums = jnp.sum(jnp.where(at[:, :, None], sums[None], 0.0), axis=1)
    sums = jnp.sum(sums, axis=0)
    load = sums[all_experts : 2 * all_experts]
    mass = sums[2 * all_experts : 3 * all_experts] + sums[3 * all_experts : 4 * all_experts]
    penalty = all_experts * jnp.sum(load * mass) / (choose * float(all_tokens) * float(all_tokens))

    span = chips * tok_rows
    slots = chips * capacity
    everyone = everyone.reshape(subs, span, width)
    notes = notes.reshape(subs, span, -1)
    lanes = jnp.arange(notes.shape[2])
    owner = jnp.arange(span, dtype=jnp.int32) // tok_rows
    cells = jnp.arange(slots, dtype=jnp.int32)
    before = (jnp.arange(tok_rows)[:, None] < jnp.arange(tok_rows)[None, :]).astype(jnp.float32)
    mixed = [0.0] * subs
    for item in range(local_experts):
        column = me * local_experts + item
        weight = jnp.sum(jnp.where(lanes == column, notes, 0.0), axis=2)
        chosen = jnp.sum(jnp.where(lanes == all_experts + column, notes, 0.0), axis=2)
        rank = jnp.dot(chosen.reshape(devices, tok_rows), before).reshape(subs, span)
        spot = jnp.where(chosen > 0, rank.astype(jnp.int32) + owner * capacity, -1)
        match = spot[:, :, None] == cells
        table = match.astype(jnp.bfloat16)
        mixing = jnp.where(match, weight[:, :, None], 0.0).astype(jnp.bfloat16)
        table, mixing = lax.optimization_barrier((table, mixing))
        rows = lax.dot_general(
            table, everyone, (((1,), (1,)), ((0,), (0,))), preferred_element_type=jnp.float32
        ).astype(jnp.bfloat16).reshape(subs * slots, width)
        rows = lax.optimization_barrier(rows)
        inner = jnp.dot(rows, routed_gate_up[item], preferred_element_type=jnp.float32)
        active = (jax.nn.silu(inner[:, :hidden_units]) * inner[:, hidden_units:]).astype(
            jnp.bfloat16
        )
        active = lax.optimization_barrier(active)
        results = jnp.dot(active, routed_down[item], preferred_element_type=jnp.float32).astype(
            jnp.bfloat16
        )
        results = lax.optimization_barrier(results)
        for r in range(subs):
            mixed[r] = mixed[r] + jnp.dot(
                mixing[r], results[r * slots : (r + 1) * slots], preferred_element_type=jnp.float32
            )

    piece = everyone[0]
    gate_part = jnp.dot(piece, shared_weights[0], preferred_element_type=jnp.float32)
    up_part = jnp.dot(piece, shared_weights[1], preferred_element_type=jnp.float32)
    shared_active = (jax.nn.silu(gate_part) * up_part).astype(jnp.bfloat16)
    shared_active = lax.optimization_barrier(shared_active)
    partials = lax.dot_general(
        shared_active,
        shared_weights[2],
        (((1,), (1,)), ((), ())),
        preferred_element_type=jnp.float32,
    )
    mixed[0] = mixed[0] + partials
    parts = [part.astype(jnp.bfloat16).reshape(chips, tok_rows, width) for part in mixed]
    return (ring_scatter(parts, chips, subs, fold), penalty.reshape(1))


def fold_of(mesh):
    chips = mesh.shape["expert"]
    try:
        spots = [tuple(d.coords) for d in mesh.devices[0, :, 0].flat]
    except (AttributeError, TypeError, ValueError):
        spots = []
    if chips % 2 or chips < 4:
        return 1
    if len(spots) == chips:
        apart = sum(abs(a - b) for a, b in zip(spots[0], spots[2]))
        return 2 if apart == 1 else 1
    return 1


def solution(mesh):
    placed = (
        P(("groups", "expert", "sub"), None),
        P(),
        P(),
        P(("groups", "expert", "sub"), None),
        P(("groups", "expert", "sub")),
        P(("expert", "sub"), None, None),
        P(("expert", "sub"), None, None),
        P(None, None, "expert"),
    )
    return jax.shard_map(
        functools.partial(on_device, fold_of(mesh)),
        mesh=mesh,
        in_specs=placed,
        out_specs=(P(("groups", "expert", "sub"), None), P("groups")),
        check_vma=False,
    )
```
